32 devices in a mesh: section: 4 (over z), tensor: 4 (over y, x), dp: 2 (over core).
Axes of the slice: x: 2, y: 2, z: 4, core: 2. Of those that a mesh axis runs over, the one named last changes fastest.
Arguments:
- enc_hidden: bfloat16 [128, 2048], P(('dp', 'tensor'), 'section'), parts along dimension 0, may hold values from -70 to 70
- mlp_gain: float32 [2048], P('section'), may hold values from 0.25 to 1.75
- final_gain: float32 [2048], P('section'), may hold values from 0.25 to 1.75
- w_gate: bfloat16 [2048, 8192], P('section', 'tensor'), may hold values from -0.125 to 0.125
- w_up: bfloat16 [2048, 8192], P('section', 'tensor'), may hold values from -0.125 to 0.125
- w_down: bfloat16 [8192, 2048], P('tensor', 'section'), may hold values from -0.0625 to 0.0625
- key_weight: bfloat16 [4, 2048, 4096], P('section', None, 'tensor'), may hold values from -0.125 to 0.125
- value_weight: bfloat16 [4, 2048, 4096], P('section', None, 'tensor'), may hold values from -0.125 to 0.125
- queries: bfloat16 [4, 2048, 4096], P('section', 'dp', 'tensor'), parts along dimension 1, may hold values from -340 to 340
- context_grad: bfloat16 [4, 2048, 4096], P('section', 'dp', 'tensor'), parts along dimension 1, may hold values from -6 to 6
Outputs:
- query_grad: bfloat16 [4, 2048, 4096], P('section', 'dp', 'tensor'), parts along dimension 1
- hidden_grad: float32 [128, 2048], P(('dp', 'tensor'), 'section'), parts along dimension 0
- gate_weight_grad: bfloat16 [4096, 8192], P(('dp', 'section'), 'tensor'), parts along dimension 0
- up_weight_grad: bfloat16 [4096, 8192], P(('dp', 'section'), 'tensor'), parts along dimension 0
- down_weight_grad: bfloat16 [16384, 2048], P(('dp', 'tensor'), 'section'), parts along dimension 0
The draws below stay inside these ranges and needn't reach their ends.
There are 2 independent parts, one for each index of `dp`. The reference program is written for one: setup_inputs(seed, part) draws one part's arguments, and reference() takes and returns one part's arrays. A program takes and returns all parts, laid end to end along the dimension named above; an argument that names none is the same for every part. Nothing has to cross between parts.
All inputs are finite; a program needn't handle non-finite values.
Results may differ from the reference program's by a relative error of at most 0.017.
Values may be sent and summed in bfloat16 or wider, within the bound.
A program may use at most 64 MiB of HBM per device.

```python
import math
import jax
import jax.numpy as jnp
from jax import lax

D = 2048
FF = 8192
HEADS = 16
HEAD = 256
TGT = 1024
SRC = 64
LAYERS = 4
HD = 4096


def draw_enc_hidden(key, part):
    key_base = jax.random.fold_in(key, 11)
    key_rows = jax.random.fold_in(key, 12)
    key_cols = jax.random.fold_in(key, 13)
    col_trend = 1.0 + 2.0 * jnp.arange(D, dtype=jnp.float32)[None, :] / D
    col_scale = col_trend * jnp.exp(jax.random.uniform(key_cols, (1, D), jnp.float32, 0.0, math.log(10.0 / 3.0)))
    row_scale = 0.1 * jnp.exp(jax.random.uniform(key_rows, (SRC, 1), jnp.float32, 0.0, math.log(10.0)))
    base_draw = jnp.clip(jax.random.normal(key_base, (SRC, D), jnp.float32), -6.0, 6.0)
    return (base_draw * row_scale * col_scale).astype(jnp.bfloat16)


def draw_queries(key, part):
    key_base = jax.random.fold_in(key, 21)
    base_draw = jnp.clip(jax.random.normal(key_base, (LAYERS, TGT, HEADS * HEAD), jnp.float32), -6.0, 6.0)
    return base_draw.astype(jnp.bfloat16)


def draw_context_grad(key, part):
    key_base = jax.random.fold_in(key, 31)
    base_draw = jnp.clip(jax.random.normal(key_base, (LAYERS, TGT, HEADS * HEAD), jnp.float32), -6.0, 6.0)
    return base_draw.astype(jnp.bfloat16)


def steps_of(rng, dims, pieces, smallest, largest):
    loudness = 1.0
    for position, parts in pieces:
        steps = jax.random.uniform(jax.random.fold_in(jax.random.fold_in(rng, 6), position), (parts,), jnp.float32, smallest / len(pieces), largest / len(pieces))
        loudness = loudness * jnp.repeat(jnp.exp(steps), dims[position] // parts).reshape((-1,) + (1,) * (len(dims) - 1 - position))
    return loudness


def normal_values(stream_key, shape, deviation, most, pieces=(), kind=jnp.bfloat16):
    loudness = steps_of(stream_key, shape, pieces, -0.22, 0.18) if pieces else 1.0
    result = jax.random.normal(stream_key, shape, jnp.float32) * deviation * loudness
    return jnp.minimum(jnp.maximum(result, -most), most).astype(kind)


def setup_inputs(seed: int = 0, part: int = 0) -> dict:
    splits = jax.random.split(jax.random.key(seed), 11)
    part_keys = jax.random.split(jax.random.fold_in(splits[10], part), 11)
    enc_hidden = draw_enc_hidden(jax.random.fold_in(jax.random.fold_in(splits[10], part), 71), part)
    mlp_gain = jnp.clip(1.0 + 0.15 * jax.random.normal(splits[1], (D,), jnp.float32), 0.25, 1.75)
    final_gain = jnp.clip(1.0 + 0.15 * jax.random.normal(splits[2], (D,), jnp.float32), 0.25, 1.75)
    w_gate = normal_values(splits[3], (D, FF), D ** -0.5, 0.125, ((0, 4), (1, 4)))
    w_up = normal_values(splits[4], (D, FF), D ** -0.5, 0.125, ((0, 4), (1, 4)))
    w_down = normal_values(splits[5], (FF, D), FF ** -0.5, 0.0625, ((0, 4), (1, 4)))
    key_weight = normal_values(splits[6], (LAYERS, D, HD), D ** -0.5, 0.125, ((0, 4), (2, 4)))
    value_weight = normal_values(splits[7], (LAYERS, D, HD), D ** -0.5, 0.125, ((0, 4), (2, 4)))
    queries = draw_queries(jax.random.fold_in(jax.random.fold_in(splits[10], part), 71), part)
    context_grad = draw_context_grad(jax.random.fold_in(jax.random.fold_in(splits[10], part), 71), part)
    return {"enc_hidden": enc_hidden, "mlp_gain": mlp_gain, "final_gain": final_gain, "w_gate": w_gate, "w_up": w_up, "w_down": w_down, "key_weight": key_weight, "value_weight": value_weight, "queries": queries, "context_grad": context_grad}


EPSILON = 1e-06

def layer_pass(encoded, key_matrix, value_matrix, query_block, grad_block):
    scale_factor = HEAD ** (-0.5)
    keys = jnp.dot(encoded, key_matrix, preferred_element_type=jnp.float32).astype(jnp.bfloat16)
    values = jnp.dot(encoded, value_matrix, preferred_element_type=jnp.float32).astype(jnp.bfloat16)
    src_rows = keys.shape[0]
    tgt_rows = query_block.shape[0]
    query_heads = query_block.reshape(tgt_rows, HEADS, HEAD).astype(jnp.float32)
    key_heads = keys.reshape(src_rows, HEADS, HEAD).astype(jnp.float32)
    value_heads = values.reshape(src_rows, HEADS, HEAD).astype(jnp.float32)
    grad_heads = grad_block.reshape(tgt_rows, HEADS, HEAD).astype(jnp.float32)
    scores = jnp.einsum('qhd,khd->hqk', query_heads, key_heads) * scale_factor
    probs = jax.nn.softmax(scores, axis=-1)
    probs_bf = probs.astype(jnp.bfloat16)
    probs_wide = probs_bf.astype(jnp.float32)
    context = jnp.einsum('hqk,khd->qhd', probs_wide, value_heads)
    delta = lax.optimization_barrier(jnp.sum(grad_heads * context, axis=2))
    dprob = jnp.einsum('qhd,khd->hqk', grad_heads, value_heads)
    dscore = (probs * (dprob - jnp.transpose(delta)[:, :, None]) * scale_factor).astype(jnp.bfloat16)
    dscore_wide = dscore.astype(jnp.float32)
    query_grad = jnp.einsum('hqk,khd->qhd', dscore_wide, key_heads).astype(jnp.bfloat16)
    key_grad = jnp.einsum('hqk,qhd->khd', dscore_wide, query_heads).astype(jnp.bfloat16)
    value_grad = jnp.einsum('hqk,qhd->khd', probs_wide, grad_heads).astype(jnp.bfloat16)
    key_grad = key_grad.reshape(src_rows, HEADS * HEAD)
    value_grad = value_grad.reshape(src_rows, HEADS * HEAD)
    contract = (((1,), (1,)), ((), ()))
    encoded_grad = lax.dot_general(key_grad, key_matrix, contract, preferred_element_type=jnp.float32)
    encoded_grad = encoded_grad + lax.dot_general(value_grad, value_matrix, contract, preferred_element_type=jnp.float32)
    return (query_grad.reshape(tgt_rows, HEADS * HEAD), encoded_grad)

def reference(enc_hidden, mlp_gain, final_gain, w_gate, w_up, w_down, key_weight, value_weight, queries, context_grad):
    hidden_wide = enc_hidden.astype(jnp.float32)
    inv_in = lax.rsqrt(lax.optimization_barrier(jnp.mean(hidden_wide * hidden_wide, axis=1, keepdims=True)) + EPSILON)
    normed = (hidden_wide * inv_in * mlp_gain[None, :]).astype(jnp.bfloat16)
    gate_pre = jnp.dot(normed, w_gate, preferred_element_type=jnp.float32)
    up_pre = jnp.dot(normed, w_up, preferred_element_type=jnp.float32)
    sigmoid_gate = jax.nn.sigmoid(gate_pre)
    activated = gate_pre * sigmoid_gate
    hidden_act = (activated * up_pre).astype(jnp.bfloat16)
    outer = hidden_wide + jnp.dot(hidden_act, w_down, preferred_element_type=jnp.float32)
    inv_out = lax.rsqrt(lax.optimization_barrier(jnp.mean(outer * outer, axis=1, keepdims=True)) + EPSILON)
    encoded = (outer * inv_out * final_gain[None, :]).astype(jnp.bfloat16)

    def one_layer(inputs):
        return layer_pass(encoded, inputs[0], inputs[1], inputs[2], inputs[3])
    query_grad, layer_grads = lax.map(one_layer, (key_weight, value_weight, queries, context_grad))
    encoded_grad = lax.optimization_barrier(jnp.sum(layer_grads, axis=0))
    scaled_out = final_gain[None, :] * encoded_grad
    inner_out = lax.optimization_barrier(jnp.mean(scaled_out * outer, axis=1, keepdims=True))
    outer_grad = inv_out * scaled_out - outer * inv_out * inv_out * inv_out * inner_out
    outer_grad_bf = outer_grad.astype(jnp.bfloat16)
    rows_contract = (((0,), (0,)), ((), ()))
    down_weight_grad = lax.dot_general(hidden_act, outer_grad_bf, rows_contract, preferred_element_type=jnp.float32).astype(jnp.bfloat16)
    cols_contract = (((1,), (1,)), ((), ()))
    act_grad = lax.dot_general(outer_grad_bf, w_down, cols_contract, preferred_element_type=jnp.float32)
    up_grad = (act_grad * activated).astype(jnp.bfloat16)
    gate_grad = (act_grad * up_pre * sigmoid_gate * (1.0 + gate_pre * (1.0 - sigmoid_gate))).astype(jnp.bfloat16)
    gate_weight_grad = lax.dot_general(normed, gate_grad, rows_contract, preferred_element_type=jnp.float32).astype(jnp.bfloat16)
    up_weight_grad = lax.dot_general(normed, up_grad, rows_contract, preferred_element_type=jnp.float32).astype(jnp.bfloat16)
    normed_grad = lax.dot_general(gate_grad, w_gate, cols_contract, preferred_element_type=jnp.float32)
    normed_grad = normed_grad + lax.dot_general(up_grad, w_up, cols_contract, preferred_element_type=jnp.float32)
    scaled_in = mlp_gain[None, :] * normed_grad
    inner_in = lax.optimization_barrier(jnp.mean(scaled_in * hidden_wide, axis=1, keepdims=True))
    hidden_grad = outer_grad + inv_in * scaled_in - hidden_wide * inv_in * inv_in * inv_in * inner_in
    return (query_grad, hidden_grad, gate_weight_grad, up_weight_grad, down_weight_grad)
```

```python
import functools
import jax
import jax.numpy as jnp
from jax import lax
from jax.experimental import pallas as pl
from jax.experimental.pallas import tpu as pltpu
from jax.sharding import PartitionSpec as P

HEAD = 256
EPSILON = 1e-06
LANES = 128
MESH = pl.DeviceIdType.MESH
VMEM_LIMIT = 40 * 1024 * 1024
ROWS = (((0,), (0,)), ((), ()))
COLS = (((1,), (1,)), ((), ()))
F32 = jnp.float32
BF16 = jnp.bfloat16


def enter(sizes):
    barrier = pltpu.get_barrier_semaphore()
    for axis, n in sizes:
        me = lax.axis_index(axis)
        for k in range(1, n):
            pl.semaphore_signal(
                barrier, inc=1, device_id={axis: lax.rem(me + k, n)}, device_id_type=MESH
            )
    pl.semaphore_wait(barrier, sum(n - 1 for _, n in sizes))


def post(axis, n, source, target, send_sem, recv_sem):
    me = lax.axis_index(axis)
    copies = []
    for k in range(1, n):
        peer = lax.rem(me + k, n)
        copy = pltpu.make_async_remote_copy(
            src_ref=source(peer),
            dst_ref=target(k - 1),
            send_sem=send_sem.at[k - 1],
            recv_sem=recv_sem.at[k - 1],
            device_id={axis: peer},
            device_id_type=MESH,
        )
        copy.start()
        copies.append(copy)
    return copies


def gather(axis, n, ref, send_sem, recv_sem):
    me = lax.axis_index(axis)
    return post(axis, n, lambda peer: ref.at[me], lambda k: ref.at[me], send_sem, recv_sem)


def scatter(axis, n, out, into, send_sem, recv_sem):
    return post(axis, n, lambda peer: out.at[peer], lambda k: into.at[k], send_sem, recv_sem)


def finish(*groups):
    for copies in groups:
        for copy in copies:
            copy.wait()


def total(own, into, n):
    acc = own.astype(F32)
    for k in range(n - 1):
        acc = acc + into[k].astype(F32)
    return acc


def forward_kernel(
    S, N, x_ref, mg_ref, fg_ref, wg_hbm, wu_hbm, wd_hbm,
    enc_out, hid_out, normed_out, act_out, fac_out, inv_in_out, inv_out_out, outer_out,
    wg, wu, wd, xg, sqs, sqr, gus, gur, hid_all, inv_all, ds, dr, feat, sqo, enc,
    load_sem, ssem, rsem,
):
    tt, F = x_ref.shape
    T = N * tt
    ts = T // S
    H = wg.shape[1]
    D = F * S
    sec = lax.axis_index("section")
    ten = lax.axis_index("tensor")
    loads = [
        pltpu.make_async_copy(src, dst, load_sem.at[i])
        for i, (src, dst) in enumerate(((wg_hbm, wg), (wu_hbm, wu), (wd_hbm, wd)))
    ]
    for load in loads:
        load.start()
    xg[ten] = x_ref[...]
    enter((("section", S), ("tensor", N)))
    finish(post("tensor", N, lambda p: x_ref, lambda k: xg.at[ten], ssem.at[0], rsem.at[0]))
    wide = xg[...].reshape(T, F).astype(F32)
    scaled = (wide * mg_ref[...]).astype(BF16)
    square = jnp.sum(wide * wide, axis=1, keepdims=True)
    sqs[...] = jnp.broadcast_to(square, (T, LANES)).reshape(S, ts, LANES)
    loads[0].wait()
    gus[0] = jnp.dot(scaled, wg[...], preferred_element_type=F32).astype(BF16).reshape(S, ts, H)
    move_g = scatter("section", S, gus.at[0], gur.at[0], ssem.at[1], rsem.at[1])
    move_q = scatter("section", S, sqs, sqr, ssem.at[3], rsem.at[3])
    loads[1].wait()
    gus[1] = jnp.dot(scaled, wu[...], preferred_element_type=F32).astype(BF16).reshape(S, ts, H)
    move_u = scatter("section", S, gus.at[1], gur.at[1], ssem.at[2], rsem.at[2])
    finish(move_g, move_q)
    inv = lax.rsqrt(total(sqs[sec], sqr, S) / D + EPSILON)
    inv_all[sec] = inv
    move_i = gather("section", S, inv_all, ssem.at[5], rsem.at[5])
    inv = inv[:, :1]
    gate_pre = total(gus[0, sec], gur.at[0], S) * inv
    sig = jax.nn.sigmoid(gate_pre)
    act = gate_pre * sig
    act_out[...] = act
    slope = sig * (1.0 + gate_pre * (1.0 - sig))
    finish(move_u)
    up_pre = total(gus[1, sec], gur.at[1], S) * inv
    hid_all[sec] = (act * up_pre).astype(BF16)
    move_h = gather("section", S, hid_all, ssem.at[4], rsem.at[4])
    fac_out[...] = up_pre * slope
    finish(move_i)
    inv_tok = inv_all[...].reshape(T, LANES)
    normed_out[...] = (wide * inv_tok[:, :1] * mg_ref[...]).astype(BF16)
    inv_flat = inv_all.reshape(T, LANES)
    inv_in_out[...] = inv_flat[pl.ds(pl.multiple_of(ten * tt, tt), tt), :]
    loads[2].wait()
    finish(move_h)
    hid = hid_all[...].reshape(T, H)
    ds[...] = jnp.dot(hid, wd[...], preferred_element_type=F32).astype(BF16).reshape(N, tt, F)
    move_d = scatter("tensor", N, ds, dr, ssem.at[6], rsem.at[6])
    hid_out[...] = hid
    finish(move_d)
    outer = x_ref[...].astype(F32) + total(ds[ten], dr, N)
    outer_out[...] = outer
    feat[sec] = (outer * fg_ref[...]).astype(BF16)
    sqo[sec] = jnp.broadcast_to(jnp.sum(outer * outer, axis=1, keepdims=True), (tt, LANES))
    move_s = gather("section", S, sqo, ssem.at[8], rsem.at[8])
    move_f = gather("section", S, feat, ssem.at[7], rsem.at[7])
    finish(move_s, move_f)
    inv_o = lax.rsqrt(jnp.sum(sqo[...], axis=0) / D + EPSILON)
    inv_out_out[...] = inv_o
    enc[ten] = (feat[...].astype(F32) * inv_o[None, :, :1]).astype(BF16)
    finish(gather("tensor", N, enc, ssem.at[9], rsem.at[9]))
    enc_out[...] = enc[...]


def attention_kernel(S, N, enc_ref, wk_ref, wv_ref, q_ref, c_ref, qg_ref, eg_ref, acc):
    step = pl.program_id(0)
    tt, F = enc_ref.shape[2:]
    T = N * tt
    scale = HEAD ** (-0.5)
    keys = jnp.zeros((T, HEAD), F32)
    values = jnp.zeros((T, HEAD), F32)
    for s in range(S):
        block = enc_ref[:, s].reshape(T, F)
        keys += jnp.dot(block, wk_ref[s * F : (s + 1) * F, :], preferred_element_type=F32)
        values += jnp.dot(block, wv_ref[s * F : (s + 1) * F, :], preferred_element_type=F32)
    keys = keys.astype(BF16)
    values = values.astype(BF16)
    q = q_ref[...]
    c = c_ref[...]
    scores = lax.dot_general(keys, q, COLS, preferred_element_type=F32) * scale
    weights = jnp.exp(scores - jnp.max(scores, axis=0, keepdims=True))
    probs = weights / jnp.sum(weights, axis=0, keepdims=True)
    probs_bf = probs.astype(BF16)
    dprob = lax.dot_general(values, c, COLS, preferred_element_type=F32)
    delta = jnp.sum(probs_bf.astype(F32) * dprob, axis=0, keepdims=True)
    dscore = (probs * (dprob - delta) * scale).astype(BF16)
    qg_ref[...] = lax.dot_general(dscore, keys, ROWS, preferred_element_type=F32).astype(BF16)
    key_grad = jnp.dot(dscore, q, preferred_element_type=F32).astype(BF16)
    value_grad = jnp.dot(probs_bf, c, preferred_element_type=F32).astype(BF16)
    for s in range(S):
        rows = slice(s * F, (s + 1) * F)
        part = lax.dot_general(key_grad, wk_ref[rows, :], COLS, preferred_element_type=F32)
        part += lax.dot_general(value_grad, wv_ref[rows, :], COLS, preferred_element_type=F32)

        @pl.when(step == 0)
        def _():
            acc[s] = part

        @pl.when(step > 0)
        def _():
            acc[s] += part

    @pl.when(step == pl.num_programs(0) - 1)
    def _():
        for s in range(S):
            eg_ref[:, s] = acc[s].astype(BF16).reshape(N, tt, F)


def backward_kernel(
    S, N, eg_ref, x_ref, mg_ref, fg_ref, act_ref, fac_ref, inv_in_ref, inv_out_ref, outer_ref,
    wg_hbm, wu_hbm, wd_hbm,
    hg_out, oall_out, gate_out, up_out,
    wg, wu, wd, r6, s6, r6b, pin, oall, s9, r9, ggu, s11, r11, pin2,
    load_sem, ssem, rsem,
):
    tt, F = x_ref.shape
    T = N * tt
    ts = T // S
    H = wg.shape[1]
    D = F * S
    sec = lax.axis_index("section")
    ten = lax.axis_index("tensor")
    loads = [
        pltpu.make_async_copy(src, dst, load_sem.at[i])
        for i, (src, dst) in enumerate(((wd_hbm, wd), (wg_hbm, wg), (wu_hbm, wu)))
    ]
    for load in loads:
        load.start()
    enter((("section", S), ("tensor", N)))
    finish(scatter("tensor", N, eg_ref, r6, ssem.at[0], rsem.at[0]))
    s6[...] = total(eg_ref[ten], r6, N).astype(BF16)
    finish(scatter("section", S, s6, r6b, ssem.at[1], rsem.at[1]))
    outer = outer_ref[...]
    scaled_out = fg_ref[...] * total(s6[sec], r6b, S)
    pin[sec] = jnp.broadcast_to(
        jnp.sum(scaled_out * outer, axis=1, keepdims=True), (tt, LANES)
    )
    finish(gather("section", S, pin, ssem.at[2], rsem.at[2]))
    inner = jnp.sum(pin[...], axis=0)[:, :1] / D
    inv_o = inv_out_ref[:, :1]
    outer_grad = inv_o * scaled_out - outer * (inv_o * inv_o * inv_o * inner)
    oall[ten] = outer_grad.astype(BF16)
    finish(gather("tensor", N, oall, ssem.at[3], rsem.at[3]))
    grads = oall[...].reshape(T, F)
    loads[0].wait()
    s9[...] = (
        lax.dot_general(grads, wd[...], COLS, preferred_element_type=F32)
        .astype(BF16)
        .reshape(S, ts, H)
    )
    move_a = scatter("section", S, s9, r9, ssem.at[4], rsem.at[4])
    oall_out[...] = grads
    finish(move_a)
    act_grad = total(s9[sec], r9, S)
    ggu[0, sec] = (act_grad * fac_ref[...]).astype(BF16)
    move_g = gather("section", S, ggu.at[0], ssem.at[5], rsem.at[5])
    ggu[1, sec] = (act_grad * act_ref[...]).astype(BF16)
    move_u = gather("section", S, ggu.at[1], ssem.at[6], rsem.at[6])
    loads[1].wait()
    finish(move_g)
    gate_all = ggu[0].reshape(T, H)
    gate_out[...] = gate_all
    part = lax.dot_general(gate_all, wg[...], COLS, preferred_element_type=F32)
    loads[2].wait()
    finish(move_u)
    up_all = ggu[1].reshape(T, H)
    part += lax.dot_general(up_all, wu[...], COLS, preferred_element_type=F32)
    s11[...] = part.astype(BF16).reshape(N, tt, F)
    move_n = scatter("tensor", N, s11, r11, ssem.at[7], rsem.at[7])
    up_out[...] = up_all
    finish(move_n)
    hidden = x_ref[...].astype(F32)
    scaled_in = mg_ref[...] * total(s11[ten], r11, N)
    pin2[sec] = jnp.broadcast_to(
        jnp.sum(scaled_in * hidden, axis=1, keepdims=True), (tt, LANES)
    )
    finish(gather("section", S, pin2, ssem.at[8], rsem.at[8]))
    inner_in = jnp.sum(pin2[...], axis=0)[:, :1] / D
    inv_in = inv_in_ref[:, :1]
    hg_out[...] = (
        outer_grad + inv_in * scaled_in - hidden * (inv_in * inv_in * inv_in * inner_in)
    )


def on_device(
    S, N, enc_hidden, mlp_gain, final_gain, w_gate, w_up, w_down, key_weight, value_weight,
    queries, context_grad,
):
    tt, F = enc_hidden.shape
    T = N * tt
    ts = T // S
    H = w_gate.shape[1]
    peers = max(S, N) - 1
    vmem = pl.BlockSpec(memory_space=pltpu.VMEM)
    hbm = pl.BlockSpec(memory_space=pl.ANY)
    shape = jax.ShapeDtypeStruct
    dma = pltpu.SemaphoreType.DMA
    mg = mlp_gain[None, :]
    fg = final_gain[None, :]
    weights = [pltpu.VMEM(w_gate.shape, BF16), pltpu.VMEM(w_up.shape, BF16),
               pltpu.VMEM(w_down.shape, BF16)]
    enc, hid, normed, act, fac, inv_in, inv_out, outer = pl.pallas_call(
        functools.partial(forward_kernel, S, N),
        out_shape=[
            shape((N, S, tt, F), BF16), shape((T, H), BF16), shape((T, F), BF16),
            shape((ts, H), F32), shape((ts, H), F32), shape((tt, LANES), F32),
            shape((tt, LANES), F32), shape((tt, F), F32),
        ],
        in_specs=[vmem] * 3 + [hbm] * 3,
        out_specs=[vmem] * 8,
        scratch_shapes=weights + [
            pltpu.VMEM((N, tt, F), BF16),
            pltpu.VMEM((S, ts, LANES), F32),
            pltpu.VMEM((S - 1, ts, LANES), F32),
            pltpu.VMEM((2, S, ts, H), BF16),
            pltpu.VMEM((2, S - 1, ts, H), BF16),
            pltpu.VMEM((S, ts, H), BF16),
            pltpu.VMEM((S, ts, LANES), F32),
            pltpu.VMEM((N, tt, F), BF16),
            pltpu.VMEM((N - 1, tt, F), BF16),
            pltpu.VMEM((S, tt, F), BF16),
            pltpu.VMEM((S, tt, LANES), F32),
            pltpu.VMEM((N, S, tt, F), BF16),
            dma((3,)), dma((10, peers)), dma((10, peers)),
        ],
        compiler_params=pltpu.CompilerParams(
            collective_id=0, has_side_effects=True, vmem_limit_bytes=VMEM_LIMIT
        ),
    )(enc_hidden, mg, fg, w_gate, w_up, w_down)

    wk, wv, q, c = key_weight[0], value_weight[0], queries[0], context_grad[0]
    D = wk.shape[0]
    rows = q.shape[0]
    heads = q.shape[1] // HEAD
    column = lambda depth: pl.BlockSpec((depth, HEAD), lambda h: (0, h))
    whole = pl.BlockSpec((N, S, tt, F), lambda h: (0, 0, 0, 0))
    query_grad, eg = pl.pallas_call(
        functools.partial(attention_kernel, S, N),
        grid=(heads,),
        out_shape=[shape(q.shape, BF16), shape((N, S, tt, F), BF16)],
        in_specs=[whole, column(D), column(D), column(rows), column(rows)],
        out_specs=[column(rows), whole],
        scratch_shapes=[pltpu.VMEM((S, T, F), F32)],
        compiler_params=pltpu.CompilerParams(
            dimension_semantics=("arbitrary",), vmem_limit_bytes=VMEM_LIMIT
        ),
    )(enc, wk, wv, q, c)

    hidden_grad, outer_all, gate_all, up_all = pl.pallas_call(
        functools.partial(backward_kernel, S, N),
        out_shape=[shape((tt, F), F32), shape((T, F), BF16), shape((T, H), BF16),
                   shape((T, H), BF16)],
        in_specs=[vmem] * 9 + [hbm] * 3,
        out_specs=[vmem] * 4,
        scratch_shapes=weights + [
            pltpu.VMEM((N - 1, S, tt, F), BF16),
            pltpu.VMEM((S, tt, F), BF16),
            pltpu.VMEM((S - 1, tt, F), BF16),
            pltpu.VMEM((S, tt, LANES), F32),
            pltpu.VMEM((N, tt, F), BF16),
            pltpu.VMEM((S, ts, H), BF16),
            pltpu.VMEM((S - 1, ts, H), BF16),
            pltpu.VMEM((2, S, ts, H), BF16),
            pltpu.VMEM((N, tt, F), BF16),
            pltpu.VMEM((N - 1, tt, F), BF16),
            pltpu.VMEM((S, tt, LANES), F32),
            dma((3,)), dma((9, peers)), dma((9, peers)),
        ],
        compiler_params=pltpu.CompilerParams(
            collective_id=1, has_side_effects=True, vmem_limit_bytes=VMEM_LIMIT
        ),
    )(eg, enc_hidden, mg, fg, act, fac, inv_in, inv_out, outer, w_gate, w_up, w_down)

    outer_product = lambda a, b: lax.dot_general(
        a, b, ROWS, preferred_element_type=F32
    ).astype(BF16)
    return (
        query_grad[None, :, :],
        hidden_grad,
        outer_product(normed, gate_all),
        outer_product(normed, up_all),
        outer_product(hid, outer_all),
    )


def solution(mesh):
    in_specs = (
        P(("dp", "tensor"), "section"),
        P("section"),
        P("section"),
        P("section", "tensor"),
        P("section", "tensor"),
        P("tensor", "section"),
        P("section", None, "tensor"),
        P("section", None, "tensor"),
        P("section", "dp", "tensor"),
        P("section", "dp", "tensor"),
    )
    out_specs = (
        P("section", "dp", "tensor"),
        P(("dp", "tensor"), "section"),
        P(("dp", "section"), "tensor"),
        P(("dp", "section"), "tensor"),
        P(("dp", "tensor"), "section"),
    )
    body = functools.partial(on_device, mesh.shape["section"], mesh.shape["tensor"])
    return jax.shard_map(
        body, mesh=mesh, in_specs=in_specs, out_specs=out_specs, check_vma=False
    )
```

```python
import functools
import jax
import jax.numpy as jnp
from jax import lax
from jax.experimental import pallas as pl
from jax.experimental.pallas import tpu as pltpu
from jax.sharding import PartitionSpec as P

HEAD = 256
EPSILON = 1e-06
LANES = 128
MESH = pl.DeviceIdType.MESH
VMEM_LIMIT = 58 * 1024 * 1024
ROWS = (((0,), (0,)), ((), ()))
COLS = (((1,), (1,)), ((), ()))
F32 = jnp.float32
BF16 = jnp.bfloat16


def enter(sizes):
    barrier = pltpu.get_barrier_semaphore()
    for axis, n in sizes:
        me = lax.axis_index(axis)
        for k in range(1, n):
            pl.semaphore_signal(
                barrier, inc=1, device_id={axis: lax.rem(me + k, n)}, device_id_type=MESH
            )
    pl.semaphore_wait(barrier, sum(n - 1 for _, n in sizes))


def post(axis, n, source, target, send_sem, recv_sem):
    me = lax.axis_index(axis)
    copies = []
    for k in range(1, n):
        peer = lax.rem(me + k, n)
        copy = pltpu.make_async_remote_copy(
            src_ref=source(peer),
            dst_ref=target(k - 1),
            send_sem=send_sem.at[k - 1],
            recv_sem=recv_sem.at[k - 1],
            device_id={axis: peer},
            device_id_type=MESH,
        )
        copy.start()
        copies.append(copy)
    return copies


def gather(axis, n, ref, send_sem, recv_sem):
    me = lax.axis_index(axis)
    return post(axis, n, lambda peer: ref.at[me], lambda k: ref.at[me], send_sem, recv_sem)


def scatter(axis, n, out, into, send_sem, recv_sem):
    return post(axis, n, lambda peer: out.at[peer], lambda k: into.at[k], send_sem, recv_sem)


def finish(*groups):
    for copies in groups:
        for copy in copies:
            copy.wait()


def total(own, into, n):
    acc = own.astype(F32)
    for k in range(n - 1):
        acc = acc + into[k].astype(F32)
    return acc


def attend(keys, values, q, c):
    scale = HEAD ** (-0.5)
    scores = lax.dot_general(keys, q, COLS, preferred_element_type=F32) * scale
    weights = jnp.exp(scores - jnp.max(scores, axis=0, keepdims=True))
    probs = weights / jnp.sum(weights, axis=0, keepdims=True)
    probs_bf = probs.astype(BF16)
    dprob = lax.dot_general(values, c, COLS, preferred_element_type=F32)
    delta = jnp.sum(probs_bf.astype(F32) * dprob, axis=0, keepdims=True)
    dscore = (probs * (dprob - delta) * scale).astype(BF16)
    query_grad = lax.dot_general(dscore, keys, ROWS, preferred_element_type=F32).astype(BF16)
    key_grad = jnp.dot(dscore, q, preferred_element_type=F32).astype(BF16)
    value_grad = jnp.dot(probs_bf, c, preferred_element_type=F32).astype(BF16)
    return query_grad, key_grad, value_grad


def step_kernel(
    S, N, x_ref, mg_ref, fg_ref, wg_hbm, wu_hbm, wd_hbm, wk_hbm, wv_hbm, q_hbm, c_hbm,
    qg_hbm, hg_out, normed_out, hid_out, oall_out, gate_out, up_out,
    wg, wu, wd, wk, wv, q, c, qg,
    xg, sqs, sqr, gus, gur, hid_all, inv_all, ds, dr, feat, sqo, enc, af, eg,
    r6, s6, r6b, pin, oall, s9, r9, aall, s11, r11, pin2,
    load_sem, store_sem, ssem, rsem,
):
    tt, F = x_ref.shape
    T = N * tt
    ts = T // S
    H = wg.shape[1]
    D = F * S
    heads = q.shape[1] // HEAD
    sec = lax.axis_index("section")
    ten = lax.axis_index("tensor")
    loads = [
        pltpu.make_async_copy(src, dst, load_sem.at[i])
        for i, (src, dst) in enumerate((
            (wg_hbm, wg), (wu_hbm, wu), (wd_hbm, wd), (wk_hbm, wk), (wv_hbm, wv),
            (q_hbm, q), (c_hbm, c),
        ))
    ]
    for load in loads[:3]:
        load.start()
    xg[ten] = x_ref[...]
    enter((("section", S), ("tensor", N)))
    finish(post("tensor", N, lambda p: x_ref, lambda k: xg.at[ten], ssem.at[0], rsem.at[0]))
    wide = xg[...].reshape(T, F).astype(F32)
    scaled = (wide * mg_ref[...]).astype(BF16)
    square = jnp.sum(wide * wide, axis=1, keepdims=True)
    sqs[...] = jnp.broadcast_to(square, (T, LANES)).reshape(S, ts, LANES)
    loads[0].wait()
    gus[0] = jnp.dot(scaled, wg[...], preferred_element_type=F32).astype(BF16).reshape(S, ts, H)
    move_q = scatter("section", S, sqs, sqr, ssem.at[3], rsem.at[3])
    move_g = scatter("section", S, gus.at[0], gur.at[0], ssem.at[1], rsem.at[1])
    loads[1].wait()
    gus[1] = jnp.dot(scaled, wu[...], preferred_element_type=F32).astype(BF16).reshape(S, ts, H)
    move_u = scatter("section", S, gus.at[1], gur.at[1], ssem.at[2], rsem.at[2])
    for load in loads[3:]:
        load.start()
    finish(move_q, move_g)
    inv = lax.rsqrt(total(sqs[sec], sqr, S) / D + EPSILON)
    inv_all[sec] = inv
    inv = inv[:, :1]
    gate_pre = total(gus[0, sec], gur.at[0], S) * inv
    sig = jax.nn.sigmoid(gate_pre)
    act = gate_pre * sig
    af[0, sec] = act.astype(BF16)
    slope = sig * (1.0 + gate_pre * (1.0 - sig))
    finish(move_u)
    up_pre = total(gus[1, sec], gur.at[1], S) * inv
    hid_all[sec] = (act * up_pre).astype(BF16)
    move_h = gather("section", S, hid_all, ssem.at[4], rsem.at[4])
    move_i = gather("section", S, inv_all, ssem.at[5], rsem.at[5])
    af[1, sec] = (up_pre * slope).astype(BF16)
    loads[2].wait()
    finish(move_h)
    hid = hid_all[...].reshape(T, H)
    ds[...] = jnp.dot(hid, wd[...], preferred_element_type=F32).astype(BF16).reshape(N, tt, F)
    move_d = scatter("tensor", N, ds, dr, ssem.at[6], rsem.at[6])
    hid_out[...] = hid
    finish(move_i)
    inv_tok = inv_all[...].reshape(T, LANES)
    normed_out[...] = (wide * inv_tok[:, :1] * mg_ref[...]).astype(BF16)
    finish(move_d)
    outer = x_ref[...].astype(F32) + total(ds[ten], dr, N)
    feat[sec] = (outer * fg_ref[...]).astype(BF16)
    sqo[sec] = jnp.broadcast_to(jnp.sum(outer * outer, axis=1, keepdims=True), (tt, LANES))
    move_s = gather("section", S, sqo, ssem.at[8], rsem.at[8])
    move_f = gather("section", S, feat, ssem.at[7], rsem.at[7])
    finish(move_s, move_f)
    move_act = gather("section", S, af.at[0], ssem.at[10], rsem.at[10])
    move_fac = gather("section", S, af.at[1], ssem.at[11], rsem.at[11])
    inv_o = lax.rsqrt(jnp.sum(sqo[...], axis=0) / D + EPSILON)
    enc[ten] = (feat[...].astype(F32) * inv_o[None, :, :1]).astype(BF16)
    inv_o = inv_o[:, :1]
    move_e = gather("tensor", N, enc, ssem.at[9], rsem.at[9])
    for load in loads[3:]:
        load.wait()
    finish(move_e)

    width = heads * HEAD
    keys = jnp.zeros((T, width), F32)
    values = jnp.zeros((T, width), F32)
    for s in range(S):
        block = enc[:, s].reshape(T, F)
        keys += jnp.dot(block, wk[s * F : (s + 1) * F, :], preferred_element_type=F32)
        values += jnp.dot(block, wv[s * F : (s + 1) * F, :], preferred_element_type=F32)
    keys = keys.astype(BF16)
    values = values.astype(BF16)
    key_grads, value_grads, stores = [], [], []
    for h in range(heads):
        cols = slice(h * HEAD, (h + 1) * HEAD)
        query_grad, key_grad, value_grad = attend(
            keys[:, cols], values[:, cols], q[:, cols], c[:, cols]
        )
        qg[h] = query_grad
        store = pltpu.make_async_copy(qg.at[h], qg_hbm.at[:, cols], store_sem.at[h])
        store.start()
        stores.append(store)
        key_grads.append(key_grad)
        value_grads.append(value_grad)
    key_grad = jnp.concatenate(key_grads, axis=1)
    value_grad = jnp.concatenate(value_grads, axis=1)
    for s in range(S):
        rows = slice(s * F, (s + 1) * F)
        part = lax.dot_general(key_grad, wk[rows, :], COLS, preferred_element_type=F32)
        part += lax.dot_general(value_grad, wv[rows, :], COLS, preferred_element_type=F32)
        eg[:, s] = part.astype(BF16).reshape(N, tt, F)

    finish(scatter("tensor", N, eg, r6, ssem.at[12], rsem.at[12]))
    s6[...] = total(eg[ten], r6, N).astype(BF16)
    finish(scatter("section", S, s6, r6b, ssem.at[13], rsem.at[13]))
    scaled_out = fg_ref[...] * total(s6[sec], r6b, S)
    pin[sec] = jnp.broadcast_to(
        jnp.sum(scaled_out * outer, axis=1, keepdims=True), (tt, LANES)
    )
    finish(gather("section", S, pin, ssem.at[14], rsem.at[14]))
    inner = jnp.sum(pin[...], axis=0)[:, :1] / D
    outer_grad = inv_o * scaled_out - outer * (inv_o * inv_o * inv_o * inner)
    oall[ten] = outer_grad.astype(BF16)
    finish(gather("tensor", N, oall, ssem.at[15], rsem.at[15]))
    grads = oall[...].reshape(T, F)
    half = H // 2
    moves = []
    for i in range(2):
        s9[i] = (
            lax.dot_general(
                grads, wd[i * half : (i + 1) * half, :], COLS, preferred_element_type=F32
            )
            .astype(BF16)
            .reshape(S, ts, half)
        )
        moves.append(scatter("section", S, s9.at[i], r9.at[i], ssem.at[16 + i], rsem.at[16 + i]))
    oall_out[...] = grads
    finish(move_act, move_fac)
    gathers = []
    for i in range(2):
        finish(moves[i])
        aall[i, sec] = total(s9[i, sec], r9.at[i], S).astype(BF16)
        gathers.append(gather("section", S, aall.at[i], ssem.at[18 + i], rsem.at[18 + i]))
    parts = None
    for i in range(2):
        cols = slice(i * half, (i + 1) * half)
        finish(gathers[i])
        act_grad = aall[i].reshape(T, half).astype(F32)
        up_grad = (act_grad * af[0, :, :, cols].reshape(T, half).astype(F32)).astype(BF16)
        gate_grad = (act_grad * af[1, :, :, cols].reshape(T, half).astype(F32)).astype(BF16)
        up_out[:, cols] = up_grad
        gate_out[:, cols] = gate_grad
        part = lax.dot_general(gate_grad, wg[:, cols], COLS, preferred_element_type=F32)
        part += lax.dot_general(up_grad, wu[:, cols], COLS, preferred_element_type=F32)
        parts = part if parts is None else parts + part
    s11[...] = parts.astype(BF16).reshape(N, tt, F)
    finish(scatter("tensor", N, s11, r11, ssem.at[20], rsem.at[20]))
    hidden = x_ref[...].astype(F32)
    scaled_in = mg_ref[...] * total(s11[ten], r11, N)
    pin2[sec] = jnp.broadcast_to(
        jnp.sum(scaled_in * hidden, axis=1, keepdims=True), (tt, LANES)
    )
    finish(gather("section", S, pin2, ssem.at[21], rsem.at[21]))
    inner_in = jnp.sum(pin2[...], axis=0)[:, :1] / D
    inv_flat = inv_all.reshape(T, LANES)
    inv_in = inv_flat[pl.ds(pl.multiple_of(ten * tt, tt), tt), :][:, :1]
    hg_out[...] = (
        outer_grad + inv_in * scaled_in - hidden * (inv_in * inv_in * inv_in * inner_in)
    )
    for store in stores:
        store.wait()


def on_device(
    S, N, enc_hidden, mlp_gain, final_gain, w_gate, w_up, w_down, key_weight, value_weight,
    queries, context_grad,
):
    tt, F = enc_hidden.shape
    T = N * tt
    ts = T // S
    H = w_gate.shape[1]
    peers = max(S, N) - 1
    vmem = pl.BlockSpec(memory_space=pltpu.VMEM)
    hbm = pl.BlockSpec(memory_space=pl.ANY)
    shape = jax.ShapeDtypeStruct
    dma = pltpu.SemaphoreType.DMA
    wk, wv, q, c = key_weight[0], value_weight[0], queries[0], context_grad[0]
    large = (w_gate, w_up, w_down, wk, wv, q, c)
    rows = q.shape[0]
    heads = q.shape[1] // HEAD
    scratch = [pltpu.VMEM(w.shape, BF16) for w in large]
    scratch += [
        pltpu.VMEM((heads, rows, HEAD), BF16),
        pltpu.VMEM((N, tt, F), BF16),
        pltpu.VMEM((S, ts, LANES), F32),
        pltpu.VMEM((S - 1, ts, LANES), F32),
        pltpu.VMEM((2, S, ts, H), BF16),
        pltpu.VMEM((2, S - 1, ts, H), BF16),
        pltpu.VMEM((S, ts, H), BF16),
        pltpu.VMEM((S, ts, LANES), F32),
        pltpu.VMEM((N, tt, F), BF16),
        pltpu.VMEM((N - 1, tt, F), BF16),
        pltpu.VMEM((S, tt, F), BF16),
        pltpu.VMEM((S, tt, LANES), F32),
        pltpu.VMEM((N, S, tt, F), BF16),
        pltpu.VMEM((2, S, ts, H), BF16),
        pltpu.VMEM((N, S, tt, F), BF16),
        pltpu.VMEM((N - 1, S, tt, F), BF16),
        pltpu.VMEM((S, tt, F), BF16),
        pltpu.VMEM((S - 1, tt, F), BF16),
        pltpu.VMEM((S, tt, LANES), F32),
        pltpu.VMEM((N, tt, F), BF16),
        pltpu.VMEM((2, S, ts, H // 2), BF16),
        pltpu.VMEM((2, S - 1, ts, H // 2), BF16),
        pltpu.VMEM((2, S, ts, H // 2), BF16),
        pltpu.VMEM((N, tt, F), BF16),
        pltpu.VMEM((N - 1, tt, F), BF16),
        pltpu.VMEM((S, tt, LANES), F32),
        dma((7,)), dma((heads,)), dma((22, peers)), dma((22, peers)),
    ]
    query_grad, hidden_grad, normed, hid, outer_all, gate_all, up_all = pl.pallas_call(
        functools.partial(step_kernel, S, N),
        out_shape=[
            shape(q.shape, BF16), shape((tt, F), F32), shape((T, F), BF16),
            shape((T, H), BF16), shape((T, F), BF16), shape((T, H), BF16), shape((T, H), BF16),
        ],
        in_specs=[vmem] * 3 + [hbm] * 7,
        out_specs=[hbm] + [vmem] * 6,
        scratch_shapes=scratch,
        compiler_params=pltpu.CompilerParams(
            collective_id=0, has_side_effects=True, vmem_limit_bytes=VMEM_LIMIT
        ),
    )(enc_hidden, mlp_gain[None, :], final_gain[None, :], *large)

    outer_product = lambda a, b: lax.dot_general(
        a, b, ROWS, preferred_element_type=F32
    ).astype(BF16)
    return (
        query_grad[None, :, :],
        hidden_grad,
        outer_product(normed, gate_all),
        outer_product(normed, up_all),
        outer_product(hid, outer_all),
    )


def solution(mesh):
    in_specs = (
        P(("dp", "tensor"), "section"),
        P("section"),
        P("section"),
        P("section", "tensor"),
        P("section", "tensor"),
        P("tensor", "section"),
        P("section", None, "tensor"),
        P("section", None, "tensor"),
        P("section", "dp", "tensor"),
        P("section", "dp", "tensor"),
    )
    out_specs = (
        P("section", "dp", "tensor"),
        P(("dp", "tensor"), "section"),
        P(("dp", "section"), "tensor"),
        P(("dp", "section"), "tensor"),
        P(("dp", "tensor"), "section"),
    )
    body = functools.partial(on_device, mesh.shape["section"], mesh.shape["tensor"])
    return jax.shard_map(
        body, mesh=mesh, in_specs=in_specs, out_specs=out_specs, check_vma=False
    )
```
